32 devices in a mesh: cell: 8 (over z, y), inst: 4 (over x, core).
Axes of the slice: x: 2, y: 2, z: 4, core: 2. Of those that a mesh axis runs over, the one named last changes fastest.
Arguments:
- fine_residual: float32 [8, 6, 65536], P('inst', None, 'cell'), may hold values from -6 to 6
- fine_map: int32 [65536], P('cell'), may hold values from 0 to 15
- routes: int32 [8, 64], P('cell'), may hold values from 0 to 7, as said below
- receive_lists: int32 [8, 192], P('cell'), may hold values from 0 to 1023
- neighbours: int32 [6, 8192], P(None, 'cell'), may hold values from 0 to 1215, as said below
- face_weights: float32 [6, 8192], P(None, 'cell'), may hold values from 0.3 to 3
- spectral_coef: float32 [8192], P('cell'), may hold values from 0.2 to 1
- diag_extra: float32 [6, 8192], P(None, 'cell'), may hold values from 0.5 to 2
Outputs:
- fine_correction: float32 [8, 6, 65536], P('inst', None, 'cell')
- coarse_correction: float32 [8, 6, 8192], P('inst', None, 'cell')
The draws below stay inside these ranges and needn't reach their ends.
Inputs may be any that keep to these rules, and one draw needn't show every extreme that they name: `routes`: in row p, the value p appears 64 - 2 * 4 times, and (p - 1) mod 8 and (p + 1) mod 8 appear 4 times each. `receive_lists`: row o, entries t * 32 to t * 32 + 31, list cells that partition o receives as halo from partition (o + d) mod 8, with d = t - 3 for t < 3 and d = t - 2 otherwise. `neighbours`: A value below 1024 is a cell of the own partition; a value x of 1024 or more is halo slot x - 1024.
All inputs are finite; a program needn't handle non-finite values.
Results may differ from the reference program's by a relative error of at most 0.0001.
Values sent between devices are 32-bit elements; how exact they have to be, the bound alone decides.
No kernel may reach another device: no remote copies, remote signals or barrier semaphores. Data moves between devices by JAX's collectives and lax.ppermute only.
A program may use at most 64 MiB of HBM per device.

```python
import math
import jax
import jax.numpy as jnp
from jax import lax

VARS = 6
INST = 8
HB_INST = 7
NB = 6
AGG = 8
BLK = 128
RAD = 3
FB = 64
ITERS = 6
CBLK = 16
FINE = 65536
CC = 1024
COARSE = 8192
HS = 32
N_CELL = 8


def draw_routes(key, part):
    handed = FB // 16
    row_keys = jax.random.split(jax.random.fold_in(key, 17), N_CELL)

    def one_row(partition, row_key):
        slots = jnp.arange(FB, dtype=jnp.int32)
        below = jnp.mod(partition + N_CELL - 1, N_CELL)
        above = jnp.mod(partition + 1, N_CELL)
        owner_ids = jnp.where(slots < handed, below, jnp.where(slots < 2 * handed, above, partition))
        return jax.random.permutation(row_key, owner_ids)
    return jax.vmap(one_row)(jnp.arange(N_CELL, dtype=jnp.int32), row_keys).astype(jnp.int32)


def draw_neighbours(key, part):
    base = jax.random.fold_in(key, 29)
    local_key, halo_key, pick_key = jax.random.split(base, 3)
    local_ids = jax.random.randint(local_key, (NB, COARSE), 0, CC)
    halo_ids = CC + jax.random.randint(halo_key, (NB, COARSE), 0, 2 * RAD * HS)
    picked = jax.random.randint(pick_key, (NB, COARSE), 0, 5) < 4
    return jnp.where(picked, local_ids, halo_ids).astype(jnp.int32)


def touch_ends(values, rng, least, largest):
    shape = values.shape
    spot = [jax.random.randint(jax.random.fold_in(rng, axis), (), 0, shape[axis]) for axis in range(len(shape))]
    values = values.at[tuple(spot)].set(least)
    longest = shape.index(max(shape))
    spot[longest] = (spot[longest] + 1) % shape[longest]
    return values.at[tuple(spot)].set(largest)


def shard_levels(own_key, extent, cuts, low, top_value):
    def one(dim, parts):
        steps = jax.random.uniform(jax.random.fold_in(jax.random.fold_in(own_key, 6), dim), (parts,), jnp.float32, low / len(cuts), top_value / len(cuts))
        return jnp.repeat(jnp.exp(steps), extent[dim] // parts).reshape((-1,) + (1,) * (len(extent) - dim - 1))

    loudness = one(*cuts[0])
    for cut in cuts[1:]:
        loudness = loudness * one(*cut)
    return loudness


def scatter_about(rng, shape, spread, reach, pieces=(), held_as=jnp.bfloat16):
    drawn = spread * jax.random.normal(rng, shape, jnp.float32)
    if pieces:
        drawn = drawn * shard_levels(rng, shape, pieces, -0.22, 0.18)
    return jnp.clip(drawn, -reach, reach).astype(held_as)


def setup_inputs(seed: int = 0) -> dict:
    key_of = jax.random.split(jax.random.key(seed), 9)
    return {
        "fine_residual": scatter_about(key_of[0], (INST, VARS, FINE), 1.0, 6.0, ((0, 4), (2, 8)), jnp.float32),
        "fine_map": touch_ends(jax.random.randint(key_of[1], (FINE,), 0, BLK // AGG), jax.random.fold_in(key_of[1], 1), 0, (BLK // AGG) - 1).astype(jnp.int32),
        "routes": draw_routes(jax.random.fold_in(key_of[8], 71), 0),
        "receive_lists": touch_ends(jax.random.randint(key_of[3], (N_CELL, 2 * RAD * HS), 0, CC), jax.random.fold_in(key_of[3], 1), 0, CC - 1).astype(jnp.int32),
        "neighbours": draw_neighbours(jax.random.fold_in(key_of[8], 71), 0),
        "face_weights": jnp.clip(jnp.exp(math.log(3.0) - 2.3025851 * jax.random.uniform(key_of[5], (NB, COARSE), jnp.float32) ** shard_levels(key_of[5], (NB, COARSE), ((1, 8),), -0.2, 0.2)), 0.3, 3.0),
        "spectral_coef": jnp.clip(jnp.exp(math.log(1.0) - 1.609438 * jax.random.uniform(key_of[6], (COARSE,), jnp.float32) ** shard_levels(key_of[6], (COARSE,), ((0, 8),), -0.2, 0.2)), 0.2, 1.0),
        "diag_extra": jnp.clip(jnp.exp(math.log(2.0) - 1.3862944 * jax.random.uniform(key_of[7], (VARS, COARSE), jnp.float32) ** shard_levels(key_of[7], (VARS, COARSE), ((1, 8),), -0.2, 0.2)), 0.5, 2.0),
    }


exact_precision = lax.Precision.HIGHEST


def spectral_matrix():
    row_ids = jnp.arange(INST)[:, None]
    col_ids = jnp.arange(INST)[None, :]
    distance = row_ids - col_ids
    usable = (row_ids < HB_INST) & (col_ids < HB_INST) & (distance != 0)
    parity = 1.0 - 2.0 * jnp.mod(distance, 2).astype(jnp.float32)
    denominator = jnp.sin(jnp.pi * jnp.where(usable, distance, 1).astype(jnp.float32) / HB_INST)
    return jnp.where(usable, 0.5 * parity / denominator, 0.0).astype(jnp.float32)


def reference(fine_residual, fine_map, routes, receive_lists, neighbours, face_weights, spectral_coef, diag_extra):
    source = jnp.arange(N_CELL, dtype=jnp.int32)[:, None]
    relative = jnp.mod(routes - source, N_CELL)
    category = jnp.where(relative == 1, 0, jnp.where(relative == 0, 1, 2)).astype(jnp.int32)
    block_order = jnp.argsort(category, axis=1, stable=True).astype(jnp.int32)
    position = jnp.argsort(block_order, axis=1, stable=True).astype(jnp.int32)
    block_base = routes * CC + position * CBLK
    coarse_of_fine = (block_base[:, :, None] + fine_map.reshape(N_CELL, FB, BLK)).reshape(-1).astype(jnp.int32)
    flat_fine = fine_residual.reshape(INST * VARS, FINE).T
    coarse_residual = jax.ops.segment_sum(flat_fine, coarse_of_fine, num_segments=COARSE).T.reshape(INST, VARS, COARSE)
    inst_ids = jnp.arange(INST)
    coarse_residual = jnp.where((inst_ids < HB_INST)[:, None, None], coarse_residual, jnp.float32(0.0))
    owners = (jnp.arange(COARSE, dtype=jnp.int32) // CC)[None, :]
    is_local = neighbours < CC
    halo_slot = jnp.maximum(neighbours - CC, 0)
    peer_slot = halo_slot // HS
    offset = jnp.where(peer_slot < RAD, peer_slot - RAD, peer_slot - RAD + 1)
    sender = jnp.mod(owners + offset, N_CELL)
    remote_index = receive_lists[jnp.broadcast_to(owners, neighbours.shape), halo_slot]
    neighbour_ids = jnp.where(is_local, owners * CC + neighbours, sender * CC + remote_index).astype(jnp.int32)
    diagonal = jnp.sum(face_weights, axis=0)[None, :] + 3.0 * spectral_coef[None, :] + diag_extra
    spectral = spectral_matrix()
    correction = coarse_residual / diagonal[None]
    for sweep in range(ITERS):
        neighbour_sum = jnp.zeros_like(correction)
        for slot_index in range(NB):
            neighbour_sum = neighbour_sum + face_weights[slot_index][None, None, :] * jnp.take(correction, neighbour_ids[slot_index], axis=2)
        coupling = jnp.einsum("nm,mvc->nvc", spectral, correction, precision=exact_precision)
        correction = (coarse_residual + neighbour_sum - spectral_coef[None, None, :] * coupling) / diagonal[None]
    fine_correction = jnp.take(correction, coarse_of_fine, axis=2)
    return fine_correction, correction
```

```python
import jax
import jax.numpy as jnp
import numpy as np
from jax import lax
from jax.experimental import pallas as pl
from jax.experimental.pallas import tpu as pltpu
from jax.sharding import PartitionSpec as P

INST = 8
HB_INST = 7
AGG = 8
BLK = 128
RAD = 3
ITERS = 6
LANES = 128
MIB = 1024 * 1024

CBLK = BLK // AGG
PER_TILE = LANES // CBLK
OFFSETS = [slot - RAD if slot < RAD else slot - RAD + 1 for slot in range(2 * RAD)]


def fourier_basis():
    points = 2.0 * np.pi * np.arange(HB_INST) / HB_INST
    basis = np.zeros((INST, INST))
    basis[0, :HB_INST] = 1.0 / np.sqrt(HB_INST)
    for wave in range(1, INST // 2):
        basis[2 * wave, :HB_INST] = np.sqrt(2.0 / HB_INST) * np.cos(wave * points)
        basis[2 * wave + 1, :HB_INST] = np.sqrt(2.0 / HB_INST) * np.sin(wave * points)
    return basis.astype(np.float32)


def halves(value):
    high = value.astype(jnp.bfloat16)
    low = (value - high.astype(jnp.float32)).astype(jnp.bfloat16)
    return high, low


def stacked(value):
    return jnp.concatenate(halves(value), axis=0)


def dot(lhs, rhs):
    return jnp.dot(lhs, rhs, preferred_element_type=jnp.float32)


def dot_nt(lhs, rhs):
    return lax.dot_general(lhs, rhs, (((1,), (1,)), ((), ())), preferred_element_type=jnp.float32)


def block_order(routes_ref, order_ref, partition, n_cell):
    blocks = routes_ref.shape[1]
    handed = blocks // 16
    above = jnp.where(partition + 1 == n_cell, 0, partition + 1)

    def place(block, heads):
        first, own, last = heads
        route = routes_ref[0, block]
        is_own = route == partition
        is_above = route == above
        position = jnp.where(is_own, own, jnp.where(is_above, first, last))
        position = jnp.minimum(position, blocks - 1)
        order_ref[0, position] = block
        one = jnp.int32(1)
        zero = jnp.int32(0)
        return (
            first + jnp.where(is_above, one, zero),
            own + jnp.where(is_own, one, zero),
            last + jnp.where(is_own | is_above, zero, one),
        )

    lax.fori_loop(0, blocks, place, (jnp.int32(0), jnp.int32(handed), jnp.int32(blocks - handed)))


def restrict_kernel(n_cell, index_ref, routes_ref, lists_ref, fine_ref, map_ref, own_ref, send_ref, order_ref, flat_ref):
    partition = index_ref[0]
    var_count, inst_dev, _ = fine_ref.shape
    blocks = map_ref.shape[0]
    rows = var_count * inst_dev
    for var in range(var_count):
        flat_ref[var * inst_dev : (var + 1) * inst_dev, :] = fine_ref[var]
    flat_ref[rows:, :] = jnp.zeros((flat_ref.shape[0] - rows, flat_ref.shape[1]), jnp.float32)
    block_order(routes_ref, order_ref, partition, n_cell)
    height = flat_ref.shape[0]
    coarse_ids = lax.broadcasted_iota(jnp.int32, (LANES, BLK), 0)
    for tile in range(blocks // PER_TILE):
        total = jnp.zeros((2 * height, LANES), jnp.float32)
        for pair in range(PER_TILE // 2):
            values = []
            hots = []
            for place in (2 * pair, 2 * pair + 1):
                block = order_ref[0, tile * PER_TILE + place]
                values.append(flat_ref[:, pl.ds(pl.multiple_of(block * BLK, BLK), BLK)])
                target = map_ref[pl.ds(block, 1), :] + place * CBLK
                hots.append(jnp.where(coarse_ids == target, 1.0, 0.0).astype(jnp.bfloat16))
            total = total + dot_nt(stacked(jnp.concatenate(values, axis=1)), jnp.concatenate(hots, axis=1))
        own_ref[:, tile * LANES : (tile + 1) * LANES] = total[:height] + total[height:]
    lane = lax.broadcasted_iota(jnp.int32, (height, LANES), 1)
    edge = blocks // 16 * CBLK
    both = jnp.where(lane < edge, own_ref[:, :LANES], own_ref[:, own_ref.shape[1] - LANES :])
    width = send_ref.shape[2]
    lists = lists_ref[...].astype(jnp.float32)
    lists = jnp.concatenate([lists, jnp.zeros((1, width - lists.shape[1]), jnp.float32)], axis=1)
    row = lax.broadcasted_iota(jnp.int32, (height, width), 0)
    wide = jnp.concatenate([both, jnp.zeros((height, width - LANES), jnp.float32)], axis=1)
    message = jnp.where(row == rows, lists, wide)
    for target in range(n_cell):
        send_ref[target] = message


def arrive_kernel(n_cell, rows, share, index_ref, got_ref, own_ref, out_ref, pack_ref):
    partition = index_ref[0]
    below = jnp.where(partition == 0, n_cell - 1, partition - 1)
    above = jnp.where(partition + 1 == n_cell, 0, partition + 1)
    height, coarse_dev = own_ref.shape
    edge = coarse_dev // 16
    lane = lax.broadcasted_iota(jnp.int32, (height, LANES), 1)
    row = lax.broadcasted_iota(jnp.int32, (height, LANES), 0)
    first = got_ref[below][:, :LANES]
    last = got_ref[above][:, :LANES]
    out_ref[...] = own_ref[...]
    out_ref[:, :LANES] = jnp.where(row < rows, jnp.where(lane < edge, first, own_ref[:, :LANES]), 0.0)
    tail = own_ref[:, coarse_dev - LANES :]
    out_ref[:, coarse_dev - LANES :] = jnp.where(row < rows, jnp.where(lane >= LANES - edge, last, tail), 0.0)
    width = pack_ref.shape[1]
    lane = lax.broadcasted_iota(jnp.int32, (1, width), 1)
    listed = jnp.full((1, width), -1.0, jnp.float32)
    for slot, offset in enumerate(OFFSETS):
        receiver = lax.rem(partition - offset + n_cell, n_cell)
        from_receiver = got_ref[receiver][rows : rows + 1, :]
        inside = (lane >= slot * share) & (lane < (slot + 1) * share)
        listed = jnp.where(inside, from_receiver, listed)
    listed = listed.astype(jnp.int32)
    ids = lax.broadcasted_iota(jnp.int32, (coarse_dev, width), 0)
    pack_ref[...] = jnp.where(ids == listed, 1.0, 0.0).astype(jnp.bfloat16)


def matrix_kernel(neighbours_ref, weights_ref, high_ref, low_ref):
    slots, coarse_dev = neighbours_ref.shape
    step = 64
    for tile in range(coarse_dev // LANES):
        span = slice(tile * LANES, (tile + 1) * LANES)
        ids = neighbours_ref[:, span]
        weights = weights_ref[:, span]

        def chunk(block, carry):
            base = pl.multiple_of(block * step, step)
            rows = lax.broadcasted_iota(jnp.int32, (step, LANES), 0) + base
            total = jnp.zeros((step, LANES), jnp.float32)
            for slot in range(slots):
                total = total + jnp.where(rows == ids[slot : slot + 1], weights[slot : slot + 1], 0.0)
            high, low = halves(total)
            high_ref[pl.ds(base, step), span] = high
            low_ref[pl.ds(base, step), span] = low
            return carry

        lax.fori_loop(0, high_ref.shape[0] // step, chunk, 0)


def swap_pairs(value):
    height = value.shape[0]
    row = lax.broadcasted_iota(jnp.int32, value.shape, 0)
    return jnp.where(row % 2 == 0, pltpu.roll(value, height - 1, 0), pltpu.roll(value, 1, 0))


def by_parity(shape, even, odd):
    row = lax.broadcasted_iota(jnp.int32, shape, 0)
    return jnp.where(row % 2 == 0, even, odd)


def pack_halo(value, pack_ref):
    packed = dot(stacked(value), pack_ref[...])
    return packed[: value.shape[0]] + packed[value.shape[0] :]


def begin_kernel(index_ref, basis_ref, gathered_ref, weights_ref, spectral_ref, extra_ref, pack_ref,
                 start_ref, inverse_ref, coupled_ref, send_ref, diag_ref):
    pair = index_ref[1]
    groups, height, coarse_dev = gathered_ref.shape
    var_count = extra_ref.shape[0]
    value = jnp.zeros((height, coarse_dev), jnp.float32)
    shape = (height, coarse_dev)
    for group in range(groups):
        part = gathered_ref[group]
        straight = by_parity(shape, basis_ref[2 * pair, 2 * group], basis_ref[2 * pair + 1, 2 * group + 1])
        crossed = by_parity(shape, basis_ref[2 * pair, 2 * group + 1], basis_ref[2 * pair + 1, 2 * group])
        value = value + straight * part + crossed * swap_pairs(part)
    spectral = spectral_ref[...]
    shared = jnp.sum(weights_ref[...], axis=0, keepdims=True) + 3.0 * spectral
    diag_ref[...] = jnp.ones(shape, jnp.float32)
    for var in range(var_count):
        diag_ref[2 * var : 2 * var + 2, :] = jnp.broadcast_to(shared + extra_ref[var : var + 1, :], (2, coarse_dev))
    inverse = 1.0 / diag_ref[...]
    wave = pair.astype(jnp.float32)
    start = value * inverse
    start_ref[...] = start
    inverse_ref[...] = inverse
    coupled_ref[...] = by_parity(shape, wave, -wave) * spectral * inverse
    send = pack_halo(start, pack_ref)
    for target in range(send_ref.shape[0]):
        send_ref[target] = send


def new_correction(share, partition, got_ref, value, start_ref, inverse_ref, coupled_ref, high_ref, low_ref):
    n_cell, height, width = got_ref.shape
    coarse_dev = value.shape[1]
    lane = lax.broadcasted_iota(jnp.int32, (height, width), 1)
    halo = jnp.zeros((height, width), jnp.float32)
    for slot, offset in enumerate(OFFSETS):
        sender = lax.rem(partition + offset + n_cell, n_cell)
        inside = (lane >= slot * share) & (lane < (slot + 1) * share)
        halo = jnp.where(inside, got_ref[sender], halo)
    extended = stacked(jnp.concatenate([value, halo], axis=1))
    both = dot(extended, high_ref[...])
    total = both[:height] + both[height:] + dot(extended[:height], low_ref[...])
    return start_ref[...] + total * inverse_ref[...] - coupled_ref[...] * swap_pairs(value)


def sweep_kernel(share, index_ref, got_ref, value_ref, start_ref, inverse_ref, coupled_ref, high_ref, low_ref, pack_ref,
                 out_ref, send_ref):
    value = new_correction(
        share, index_ref[0], got_ref, value_ref[...], start_ref, inverse_ref, coupled_ref, high_ref, low_ref
    )
    out_ref[...] = value
    send = pack_halo(value, pack_ref)
    for target in range(send_ref.shape[0]):
        send_ref[target] = send


def last_kernel(share, index_ref, got_ref, value_ref, start_ref, inverse_ref, coupled_ref, high_ref, low_ref,
                out_ref, first_ref, last_ref):
    value = new_correction(
        share, index_ref[0], got_ref, value_ref[...], start_ref, inverse_ref, coupled_ref, high_ref, low_ref
    )
    out_ref[...] = value
    first_ref[...] = value[:, :LANES]
    last_ref[...] = value[:, value.shape[1] - LANES :]


def finish_kernel(index_ref, basis_ref, order_ref, gathered_ref, map_ref, coarse_ref, fine_ref, flat_ref):
    pair = index_ref[1]
    var_count, inst_dev, coarse_dev = coarse_ref.shape
    groups, height, wide = gathered_ref.shape
    blocks = map_ref.shape[0]
    edge = blocks // 16 * CBLK
    value = jnp.zeros((height, wide), jnp.float32)
    shape = (height, wide)
    for group in range(groups):
        part = gathered_ref[group]
        straight = by_parity(shape, basis_ref[2 * group, 2 * pair], basis_ref[2 * group + 1, 2 * pair + 1])
        crossed = by_parity(shape, basis_ref[2 * group + 1, 2 * pair], basis_ref[2 * group, 2 * pair + 1])
        value = value + straight * part + crossed * swap_pairs(part)
    for var in range(var_count):
        coarse_ref[var] = value[inst_dev * var : inst_dev * (var + 1), :coarse_dev]
    lane = lax.broadcasted_iota(jnp.int32, (height, LANES), 1)
    first_back = value[:, coarse_dev + LANES : coarse_dev + 2 * LANES]
    last_back = value[:, coarse_dev : coarse_dev + LANES]
    coarse_ids = lax.broadcasted_iota(jnp.int32, (LANES, BLK), 0)
    tiles = blocks // PER_TILE
    for tile in range(tiles):
        part = value[:, tile * LANES : (tile + 1) * LANES]
        if tile == 0:
            part = jnp.where(lane < edge, last_back, part)
        if tile == tiles - 1:
            part = jnp.where(lane >= LANES - edge, first_back, part)
        part = stacked(part)
        for pair_id in range(PER_TILE // 2):
            hots = []
            spots = []
            for place in (2 * pair_id, 2 * pair_id + 1):
                block = order_ref[0, tile * PER_TILE + place]
                target = map_ref[pl.ds(block, 1), :] + place * CBLK
                hots.append(jnp.where(coarse_ids == target, 1.0, 0.0).astype(jnp.bfloat16))
                spots.append(block)
            both = dot(part, jnp.concatenate(hots, axis=1))
            both = both[:height] + both[height:]
            for place, block in enumerate(spots):
                span = pl.ds(pl.multiple_of(block * BLK, BLK), BLK)
                flat_ref[:, span] = both[:, place * BLK : (place + 1) * BLK]
    for var in range(var_count):
        fine_ref[var] = flat_ref[inst_dev * var : inst_dev * (var + 1), :]


SMEM = pl.BlockSpec(memory_space=pltpu.SMEM)
VMEM = pl.BlockSpec(memory_space=pltpu.VMEM)


def call(kernel, outs, name, in_smem, n_in, out_smem=(), scratch=(), limit=16):
    return pl.pallas_call(
        kernel,
        name=name,
        out_shape=outs,
        in_specs=[SMEM if at in in_smem else VMEM for at in range(n_in)],
        out_specs=[SMEM if at in out_smem else VMEM for at in range(len(outs))],
        scratch_shapes=list(scratch),
        compiler_params=pltpu.CompilerParams(vmem_limit_bytes=limit * MIB),
    )


def shifted(value, axis, steps):
    count = lax.axis_size(axis)
    pairs = [(source, (source + steps) % count) for source in range(count)]
    return lax.ppermute(value, axis, pairs)


def f32(*shape):
    return jax.ShapeDtypeStruct(shape, jnp.float32)


def body(fine_residual, fine_map, routes, receive_lists, neighbours, face_weights, spectral_coef, diag_extra):
    n_cell = lax.axis_size("cell")
    inst_dev, var_count, fine_dev = fine_residual.shape
    blocks = routes.shape[1]
    coarse_dev = blocks * CBLK
    rows = inst_dev * var_count
    height = -(-(rows + 1) // 16) * 16
    halo = receive_lists.shape[1]
    halo_pad = -(-halo // 256) * 256
    share = halo // (2 * RAD)
    index = jnp.stack([lax.axis_index("cell"), lax.axis_index("inst")]).astype(jnp.int32)
    basis = jnp.asarray(fourier_basis())
    cell_map = fine_map.reshape(blocks, BLK)
    fine = fine_residual.transpose(1, 0, 2)
    spectral = spectral_coef.reshape(1, coarse_dev)

    own, send, order = call(
        lambda *refs: restrict_kernel(n_cell, *refs),
        [f32(height, coarse_dev), f32(n_cell, height, halo_pad), jax.ShapeDtypeStruct((1, blocks), jnp.int32)],
        "restrict", (0, 1), 5, (2,), [pltpu.VMEM((height, fine_dev), jnp.float32)],
    )(index, routes, receive_lists, fine, cell_map)
    got = lax.all_to_all(send, "cell", 0, 0)
    arrived, pack = call(
        lambda *refs: arrive_kernel(n_cell, rows, share, *refs),
        [f32(height, coarse_dev), jax.ShapeDtypeStruct((coarse_dev, halo_pad), jnp.bfloat16)],
        "arrive", (0,), 3,
    )(index, got, own)
    gathered = lax.all_gather(arrived, "inst", axis=0)
    half = jax.ShapeDtypeStruct((coarse_dev + halo_pad, coarse_dev), jnp.bfloat16)
    high, low = call(matrix_kernel, [half, half], "matrix", (), 2)(neighbours, face_weights)
    state = f32(height, coarse_dev)
    message = f32(n_cell, height, halo_pad)
    start, inverse, coupled, send = call(
        begin_kernel, [state, state, state, message], "begin", (0, 1), 7, (),
        [pltpu.VMEM((height, coarse_dev), jnp.float32)],
    )(index, basis, gathered, face_weights, spectral, diag_extra, pack)
    value = start
    for sweep in range(ITERS - 1):
        got = lax.all_to_all(send, "cell", 0, 0)
        value, send = call(lambda *refs: sweep_kernel(share, *refs), [state, message], "sweep", (0,), 9)(
            index, got, value, start, inverse, coupled, high, low, pack
        )
    got = lax.all_to_all(send, "cell", 0, 0)
    value, first, last = call(lambda *refs: last_kernel(share, *refs), [state, f32(height, LANES), f32(height, LANES)], "last", (0,), 8)(
        index, got, value, start, inverse, coupled, high, low
    )
    last_back = shifted(first, "cell", -1)
    first_back = shifted(last, "cell", 1)
    joined = jnp.concatenate([value, last_back, first_back], axis=1)
    gathered = lax.all_gather(joined, "inst", axis=0)
    coarse, fine_out = call(
        finish_kernel, [f32(var_count, inst_dev, coarse_dev), f32(var_count, inst_dev, fine_dev)],
        "finish", (0, 1, 2), 5, (), [pltpu.VMEM((height, fine_dev), jnp.float32)],
    )(index, basis, order, gathered, cell_map)
    return fine_out.transpose(1, 0, 2), coarse.transpose(1, 0, 2)


def solution(mesh):
    in_specs = (
        P("inst", None, "cell"),
        P("cell"),
        P("cell", None),
        P("cell", None),
        P(None, "cell"),
        P(None, "cell"),
        P("cell"),
        P(None, "cell"),
    )
    out_specs = (P("inst", None, "cell"), P("inst", None, "cell"))
    return jax.shard_map(body, mesh=mesh, in_specs=in_specs, out_specs=out_specs, check_vma=False)
```

```python
import jax
import jax.numpy as jnp
import numpy as np
from jax import lax
from jax.experimental import pallas as pl
from jax.experimental.pallas import tpu as pltpu
from jax.sharding import PartitionSpec as P

INST = 8
HB_INST = 7
AGG = 8
BLK = 128
RAD = 3
ITERS = 6
LANES = 128
MIB = 1024 * 1024

CBLK = BLK // AGG
PER_TILE = LANES // CBLK
OFFSETS = [slot - RAD if slot < RAD else slot - RAD + 1 for slot in range(2 * RAD)]


def fourier_basis():
    points = 2.0 * np.pi * np.arange(HB_INST) / HB_INST
    basis = np.zeros((INST, INST))
    basis[0, :HB_INST] = 1.0 / np.sqrt(HB_INST)
    for wave in range(1, INST // 2):
        basis[2 * wave, :HB_INST] = np.sqrt(2.0 / HB_INST) * np.cos(wave * points)
        basis[2 * wave + 1, :HB_INST] = np.sqrt(2.0 / HB_INST) * np.sin(wave * points)
    return basis.astype(np.float32)


def halves(value):
    high = value.astype(jnp.bfloat16)
    low = (value - high.astype(jnp.float32)).astype(jnp.bfloat16)
    return high, low


def stacked(value):
    return jnp.concatenate(halves(value), axis=0)


def dot(lhs, rhs):
    return jnp.dot(lhs, rhs, preferred_element_type=jnp.float32)


def dot_nt(lhs, rhs):
    return lax.dot_general(lhs, rhs, (((1,), (1,)), ((), ())), preferred_element_type=jnp.float32)


def block_order(routes_ref, order_ref, partition, n_cell):
    blocks = routes_ref.shape[1]
    handed = blocks // 16
    above = jnp.where(partition + 1 == n_cell, 0, partition + 1)

    def place(block, heads):
        first, own, last = heads
        route = routes_ref[0, block]
        is_own = route == partition
        is_above = route == above
        position = jnp.where(is_own, own, jnp.where(is_above, first, last))
        position = jnp.minimum(position, blocks - 1)
        order_ref[0, position] = block
        one = jnp.int32(1)
        zero = jnp.int32(0)
        return (
            first + jnp.where(is_above, one, zero),
            own + jnp.where(is_own, one, zero),
            last + jnp.where(is_own | is_above, zero, one),
        )

    lax.fori_loop(0, blocks, place, (jnp.int32(0), jnp.int32(handed), jnp.int32(blocks - handed)))


def restrict_kernel(n_cell, index_ref, routes_ref, lists_ref, fine_ref, map_ref, own_ref, send_ref, order_ref, flat_ref):
    partition = index_ref[0]
    var_count, inst_dev, _ = fine_ref.shape
    blocks = map_ref.shape[0]
    rows = var_count * inst_dev
    for var in range(var_count):
        flat_ref[var * inst_dev : (var + 1) * inst_dev, :] = fine_ref[var]
    flat_ref[rows:, :] = jnp.zeros((flat_ref.shape[0] - rows, flat_ref.shape[1]), jnp.float32)
    block_order(routes_ref, order_ref, partition, n_cell)
    height = flat_ref.shape[0]
    coarse_ids = lax.broadcasted_iota(jnp.int32, (LANES, BLK), 0)
    for tile in range(blocks // PER_TILE):
        total = jnp.zeros((2 * height, LANES), jnp.float32)
        for pair in range(PER_TILE // 2):
            values = []
            hots = []
            for place in (2 * pair, 2 * pair + 1):
                block = order_ref[0, tile * PER_TILE + place]
                values.append(flat_ref[:, pl.ds(pl.multiple_of(block * BLK, BLK), BLK)])
                target = map_ref[pl.ds(block, 1), :] + place * CBLK
                hots.append(jnp.where(coarse_ids == target, 1.0, 0.0).astype(jnp.bfloat16))
            total = total + dot_nt(stacked(jnp.concatenate(values, axis=1)), jnp.concatenate(hots, axis=1))
        own_ref[:, tile * LANES : (tile + 1) * LANES] = total[:height] + total[height:]
    lane = lax.broadcasted_iota(jnp.int32, (height, LANES), 1)
    edge = blocks // 16 * CBLK
    both = jnp.where(lane < edge, own_ref[:, :LANES], own_ref[:, own_ref.shape[1] - LANES :])
    width = send_ref.shape[2]
    lists = lists_ref[...].astype(jnp.float32)
    lists = jnp.concatenate([lists, jnp.zeros((1, width - lists.shape[1]), jnp.float32)], axis=1)
    row = lax.broadcasted_iota(jnp.int32, (height, width), 0)
    wide = jnp.concatenate([both, jnp.zeros((height, width - LANES), jnp.float32)], axis=1)
    message = jnp.where(row == rows, lists, wide)
    for target in range(n_cell):
        send_ref[target] = message


def arrive_kernel(n_cell, rows, share, index_ref, got_ref, own_ref, out_ref, pack_ref):
    partition = index_ref[0]
    below = jnp.where(partition == 0, n_cell - 1, partition - 1)
    above = jnp.where(partition + 1 == n_cell, 0, partition + 1)
    height, coarse_dev = own_ref.shape
    edge = coarse_dev // 16
    lane = lax.broadcasted_iota(jnp.int32, (height, LANES), 1)
    row = lax.broadcasted_iota(jnp.int32, (height, LANES), 0)
    first = got_ref[below][:, :LANES]
    last = got_ref[above][:, :LANES]
    out_ref[...] = own_ref[...]
    out_ref[:, :LANES] = jnp.where(row < rows, jnp.where(lane < edge, first, own_ref[:, :LANES]), 0.0)
    tail = own_ref[:, coarse_dev - LANES :]
    out_ref[:, coarse_dev - LANES :] = jnp.where(row < rows, jnp.where(lane >= LANES - edge, last, tail), 0.0)
    width = pack_ref.shape[1]
    lane = lax.broadcasted_iota(jnp.int32, (1, width), 1)
    listed = jnp.full((1, width), -1.0, jnp.float32)
    for slot, offset in enumerate(OFFSETS):
        receiver = lax.rem(partition - offset + n_cell, n_cell)
        from_receiver = got_ref[receiver][rows : rows + 1, :]
        inside = (lane >= slot * share) & (lane < (slot + 1) * share)
        listed = jnp.where(inside, from_receiver, listed)
    listed = listed.astype(jnp.int32)
    ids = lax.broadcasted_iota(jnp.int32, (coarse_dev, width), 0)
    pack_ref[...] = jnp.where(ids == listed, 1.0, 0.0).astype(jnp.bfloat16)


def matrix_kernel(neighbours_ref, weights_ref, high_ref, low_ref):
    slots, coarse_dev = neighbours_ref.shape
    step = 64
    for tile in range(coarse_dev // LANES):
        span = slice(tile * LANES, (tile + 1) * LANES)
        ids = neighbours_ref[:, span]
        weights = weights_ref[:, span]

        def chunk(block, carry):
            base = pl.multiple_of(block * step, step)
            rows = lax.broadcasted_iota(jnp.int32, (step, LANES), 0) + base
            total = jnp.zeros((step, LANES), jnp.float32)
            for slot in range(slots):
                total = total + jnp.where(rows == ids[slot : slot + 1], weights[slot : slot + 1], 0.0)
            high, low = halves(total)
            high_ref[pl.ds(base, step), span] = high
            low_ref[pl.ds(base, step), span] = low
            return carry

        lax.fori_loop(0, high_ref.shape[0] // step, chunk, 0)


def swap_pairs(value):
    height = value.shape[0]
    row = lax.broadcasted_iota(jnp.int32, value.shape, 0)
    return jnp.where(row % 2 == 0, pltpu.roll(value, height - 1, 0), pltpu.roll(value, 1, 0))


def by_parity(shape, even, odd):
    row = lax.broadcasted_iota(jnp.int32, shape, 0)
    return jnp.where(row % 2 == 0, even, odd)


def pack_halo(value, pack_ref):
    packed = dot(stacked(value), pack_ref[...])
    return packed[: value.shape[0]] + packed[value.shape[0] :]


def prepare_kernel(neighbours_ref, weights_ref, spectral_ref, extra_ref,
                   high_ref, low_ref, inverse_ref, coupled_ref, topology_ref):
    matrix_kernel(neighbours_ref, weights_ref, high_ref, low_ref)
    slots, coarse_dev = neighbours_ref.shape
    var_count = extra_ref.shape[0]
    weights = weights_ref[...]
    spectral = spectral_ref[...]
    diagonal = jnp.sum(weights, axis=0, keepdims=True) + 3.0 * spectral + extra_ref[...]
    inverse = 1.0 / diagonal
    inverse_ref[...] = jnp.ones(inverse_ref.shape, jnp.float32)
    for var in range(var_count):
        inverse_ref[2 * var : 2 * var + 2, :] = jnp.broadcast_to(inverse[var : var + 1], (2, coarse_dev))
    coupled_ref[...] = by_parity(coupled_ref.shape, spectral, -spectral) * inverse_ref[...]
    topology_ref[...] = jnp.zeros(topology_ref.shape, jnp.float32)
    topology_ref[0:slots, :] = neighbours_ref[...].astype(jnp.float32)
    topology_ref[8 : 8 + slots, :] = weights
    topology_ref[16 : 16 + var_count, :] = inverse


def times(value, high, low):
    height = value.shape[0]
    extended = stacked(value)
    both = dot(extended, high)
    return both[:height] + both[height:] + dot(extended[:height], low)


def local_part(value, start_ref, inverse_ref, coupled_ref, wave, high_ref, low_ref):
    coarse_dev = value.shape[1]
    total = times(value, high_ref[:coarse_dev], low_ref[:coarse_dev])
    return start_ref[...] + total * inverse_ref[...] - wave * coupled_ref[...] * swap_pairs(value)


def begin_kernel(index_ref, basis_ref, gathered_ref, inverse_ref, coupled_ref, topology_ref, pack_ref, high_ref, low_ref,
                 start_ref, local_ref, send_ref):
    pair = index_ref[1]
    groups, height, coarse_dev = gathered_ref.shape
    value = jnp.zeros((height, coarse_dev), jnp.float32)
    shape = (height, coarse_dev)
    for group in range(groups):
        part = gathered_ref[group]
        straight = by_parity(shape, basis_ref[2 * pair, 2 * group], basis_ref[2 * pair + 1, 2 * group + 1])
        crossed = by_parity(shape, basis_ref[2 * pair, 2 * group + 1], basis_ref[2 * pair + 1, 2 * group])
        value = value + straight * part + crossed * swap_pairs(part)
    start = value * inverse_ref[...]
    start_ref[...] = start
    local = local_part(start, start_ref, inverse_ref, coupled_ref, pair.astype(jnp.float32), high_ref, low_ref)
    local_ref[...] = local
    send = pack_halo(jnp.concatenate([start, local, topology_ref[...]], axis=0), pack_ref)
    for target in range(send_ref.shape[0]):
        send_ref[target] = send


def halo_of(partition, share, got_ref, top, height):
    n_cell, _, width = got_ref.shape
    lane = lax.broadcasted_iota(jnp.int32, (height, width), 1)
    halo = jnp.zeros((height, width), jnp.float32)
    for slot, offset in enumerate(OFFSETS):
        sender = lax.rem(partition + offset + n_cell, n_cell)
        inside = (lane >= slot * share) & (lane < (slot + 1) * share)
        halo = jnp.where(inside, got_ref[sender, top : top + height, :], halo)
    return halo


def double_kernel(share, first, last, slots, var_count, *refs):
    refs = list(refs)
    index_ref, got_ref, local_ref, start_ref, inverse_ref, coupled_ref, high_ref, low_ref, pack_ref = refs[:9]
    refs = refs[9:]
    if first:
        edge_ref = None
        halo_inverse_ref = None
    else:
        edge_ref, halo_inverse_ref = refs[:2]
        refs = refs[2:]
    partition = index_ref[0]
    wave = index_ref[1].astype(jnp.float32)
    n_cell, _, width = got_ref.shape
    height, coarse_dev = local_ref.shape
    out_refs = refs
    if first:
        out_refs, (edge_ref, halo_inverse_ref) = refs[:-2], refs[-2:]
        told = halo_of(partition, share, got_ref, 2 * height, 24)
        ids = told[:slots].astype(jnp.int32) - coarse_dev
        weights = told[8 : 8 + slots]
        rows = lax.broadcasted_iota(jnp.int32, (width, width), 0)
        edge = jnp.zeros((width, width), jnp.float32)
        for slot in range(slots):
            edge = edge + jnp.where(rows == ids[slot : slot + 1], weights[slot : slot + 1], 0.0)
        high, low = halves(edge)
        edge_ref[0] = high
        edge_ref[1] = low
        halo_inverse_ref[...] = jnp.zeros((height, width), jnp.float32)
        for var in range(var_count):
            halo_inverse_ref[2 * var : 2 * var + 2, :] = jnp.broadcast_to(told[16 + var : 17 + var], (2, width))
    halo_high = high_ref[coarse_dev:]
    halo_low = low_ref[coarse_dev:]
    lane = lax.broadcasted_iota(jnp.int32, (height, width), 1)
    share_of = []
    for offset in OFFSETS:
        share_of.append(halo_of(lax.rem(partition + offset + n_cell, n_cell), share, got_ref, 0, height))
    spread = times(jnp.concatenate(share_of, axis=0), edge_ref[0], edge_ref[1])
    edge_total = jnp.zeros((height, width), jnp.float32)
    for slot in range(len(OFFSETS)):
        inside = (lane >= slot * share) & (lane < (slot + 1) * share)
        edge_total = jnp.where(inside, spread[slot * height : (slot + 1) * height], edge_total)
    next_halo = halo_of(partition, share, got_ref, height, height) + halo_inverse_ref[...] * edge_total
    both = times(
        jnp.concatenate([halo_of(partition, share, got_ref, 0, height), next_halo], axis=0), halo_high, halo_low
    )
    value = local_ref[...] + both[:height] * inverse_ref[...]
    local = local_part(value, start_ref, inverse_ref, coupled_ref, wave, high_ref, low_ref)
    value = local + both[height:] * inverse_ref[...]
    if last:
        out_ref, first_ref, last_ref = out_refs
        out_ref[...] = value
        first_ref[...] = value[:, :LANES]
        last_ref[...] = value[:, coarse_dev - LANES :]
        return
    out_ref, send_ref = out_refs
    local = local_part(value, start_ref, inverse_ref, coupled_ref, wave, high_ref, low_ref)
    out_ref[...] = local
    send = pack_halo(jnp.concatenate([value, local], axis=0), pack_ref)
    for target in range(n_cell):
        send_ref[target] = send


def finish_kernel(index_ref, basis_ref, order_ref, gathered_ref, map_ref, coarse_ref, fine_ref, flat_ref):
    pair = index_ref[1]
    var_count, inst_dev, coarse_dev = coarse_ref.shape
    groups, height, wide = gathered_ref.shape
    blocks = map_ref.shape[0]
    edge = blocks // 16 * CBLK
    value = jnp.zeros((height, wide), jnp.float32)
    shape = (height, wide)
    for group in range(groups):
        part = gathered_ref[group]
        straight = by_parity(shape, basis_ref[2 * group, 2 * pair], basis_ref[2 * group + 1, 2 * pair + 1])
        crossed = by_parity(shape, basis_ref[2 * group + 1, 2 * pair], basis_ref[2 * group, 2 * pair + 1])
        value = value + straight * part + crossed * swap_pairs(part)
    for var in range(var_count):
        coarse_ref[var] = value[inst_dev * var : inst_dev * (var + 1), :coarse_dev]
    lane = lax.broadcasted_iota(jnp.int32, (height, LANES), 1)
    first_back = value[:, coarse_dev + LANES : coarse_dev + 2 * LANES]
    last_back = value[:, coarse_dev : coarse_dev + LANES]
    coarse_ids = lax.broadcasted_iota(jnp.int32, (LANES, BLK), 0)
    tiles = blocks // PER_TILE
    for tile in range(tiles):
        part = value[:, tile * LANES : (tile + 1) * LANES]
        if tile == 0:
            part = jnp.where(lane < edge, last_back, part)
        if tile == tiles - 1:
            part = jnp.where(lane >= LANES - edge, first_back, part)
        part = stacked(part)
        for pair_id in range(PER_TILE // 2):
            hots = []
            spots = []
            for place in (2 * pair_id, 2 * pair_id + 1):
                block = order_ref[0, tile * PER_TILE + place]
                target = map_ref[pl.ds(block, 1), :] + place * CBLK
                hots.append(jnp.where(coarse_ids == target, 1.0, 0.0).astype(jnp.bfloat16))
                spots.append(block)
            both = dot(part, jnp.concatenate(hots, axis=1))
            both = both[:height] + both[height:]
            for place, block in enumerate(spots):
                span = pl.ds(pl.multiple_of(block * BLK, BLK), BLK)
                flat_ref[:, span] = both[:, place * BLK : (place + 1) * BLK]
    for var in range(var_count):
        fine_ref[var] = flat_ref[inst_dev * var : inst_dev * (var + 1), :]


SMEM = pl.BlockSpec(memory_space=pltpu.SMEM)
VMEM = pl.BlockSpec(memory_space=pltpu.VMEM)


def call(kernel, outs, name, in_smem, n_in, out_smem=(), scratch=(), limit=16):
    return pl.pallas_call(
        kernel,
        name=name,
        out_shape=outs,
        in_specs=[SMEM if at in in_smem else VMEM for at in range(n_in)],
        out_specs=[SMEM if at in out_smem else VMEM for at in range(len(outs))],
        scratch_shapes=list(scratch),
        compiler_params=pltpu.CompilerParams(vmem_limit_bytes=limit * MIB),
    )


def shifted(value, axis, steps):
    count = lax.axis_size(axis)
    pairs = [(source, (source + steps) % count) for source in range(count)]
    return lax.ppermute(value, axis, pairs)


def f32(*shape):
    return jax.ShapeDtypeStruct(shape, jnp.float32)


def body(fine_residual, fine_map, routes, receive_lists, neighbours, face_weights, spectral_coef, diag_extra):
    n_cell = lax.axis_size("cell")
    inst_dev, var_count, fine_dev = fine_residual.shape
    blocks = routes.shape[1]
    coarse_dev = blocks * CBLK
    rows = inst_dev * var_count
    height = -(-(rows + 1) // 16) * 16
    halo = receive_lists.shape[1]
    halo_pad = -(-halo // 256) * 256
    share = halo // (2 * RAD)
    index = jnp.stack([lax.axis_index("cell"), lax.axis_index("inst")]).astype(jnp.int32)
    basis = jnp.asarray(fourier_basis())
    cell_map = fine_map.reshape(blocks, BLK)
    fine = fine_residual.transpose(1, 0, 2)
    spectral = spectral_coef.reshape(1, coarse_dev)

    own, send, order = call(
        lambda *refs: restrict_kernel(n_cell, *refs),
        [f32(height, coarse_dev), f32(n_cell, height, halo_pad), jax.ShapeDtypeStruct((1, blocks), jnp.int32)],
        "restrict", (0, 1), 5, (2,), [pltpu.VMEM((height, fine_dev), jnp.float32)],
    )(index, routes, receive_lists, fine, cell_map)
    got = lax.all_to_all(send, "cell", 0, 0)
    arrived, pack = call(
        lambda *refs: arrive_kernel(n_cell, rows, share, *refs),
        [f32(height, coarse_dev), jax.ShapeDtypeStruct((coarse_dev, halo_pad), jnp.bfloat16)],
        "arrive", (0,), 3,
    )(index, got, own)
    gathered = lax.all_gather(arrived, "inst", axis=0)
    slots = neighbours.shape[0]
    half = jax.ShapeDtypeStruct((coarse_dev + halo_pad, coarse_dev), jnp.bfloat16)
    state = f32(height, coarse_dev)
    high, low, inverse, coupled, topology = call(
        prepare_kernel, [half, half, state, state, f32(24, coarse_dev)], "prepare", (), 4
    )(neighbours, face_weights, spectral, diag_extra)
    start, local, send = call(
        begin_kernel, [state, state, f32(n_cell, 2 * height + 24, halo_pad)], "begin", (0, 1), 9
    )(index, basis, gathered, inverse, coupled, topology, pack, high, low)
    edges = []
    for pair in range(ITERS // 2):
        got = lax.all_to_all(send, "cell", 0, 0)
        is_first = pair == 0
        is_last = pair == ITERS // 2 - 1
        outs = [state, f32(n_cell, 2 * height, halo_pad)]
        if is_last:
            outs = [state, f32(height, LANES), f32(height, LANES)]
        if is_first:
            outs += [jax.ShapeDtypeStruct((2, halo_pad, halo_pad), jnp.bfloat16), f32(height, halo_pad)]
        outs = call(
            lambda *refs: double_kernel(share, is_first, is_last, slots, var_count, *refs),
            outs, "double", (0,), 9 + len(edges),
        )(index, got, local, start, inverse, coupled, high, low, pack, *edges)
        if is_first:
            edges = outs[-2:]
            outs = outs[:-2]
        local, *rest = outs
        if is_last:
            first, last = rest
        else:
            (send,) = rest
    value = local
    last_back = shifted(first, "cell", -1)
    first_back = shifted(last, "cell", 1)
    joined = jnp.concatenate([value, last_back, first_back], axis=1)
    gathered = lax.all_gather(joined, "inst", axis=0)
    coarse, fine_out = call(
        finish_kernel, [f32(var_count, inst_dev, coarse_dev), f32(var_count, inst_dev, fine_dev)],
        "finish", (0, 1, 2), 5, (), [pltpu.VMEM((height, fine_dev), jnp.float32)],
    )(index, basis, order, gathered, cell_map)
    return fine_out.transpose(1, 0, 2), coarse.transpose(1, 0, 2)


def solution(mesh):
    in_specs = (
        P("inst", None, "cell"),
        P("cell"),
        P("cell", None),
        P("cell", None),
        P(None, "cell"),
        P(None, "cell"),
        P("cell"),
        P(None, "cell"),
    )
    out_specs = (P("inst", None, "cell"), P("inst", None, "cell"))
    return jax.shard_map(body, mesh=mesh, in_specs=in_specs, out_specs=out_specs, check_vma=False)
```

```python
import jax
import jax.numpy as jnp
import numpy as np
from jax import lax
from jax.experimental import pallas as pl
from jax.experimental.pallas import tpu as pltpu
from jax.sharding import PartitionSpec as P

INST = 8
HB_INST = 7
AGG = 8
BLK = 128
RAD = 3
ITERS = 6
LANES = 128
MIB = 1024 * 1024

CBLK = BLK // AGG
PER_TILE = LANES // CBLK
OFFSETS = [slot - RAD if slot < RAD else slot - RAD + 1 for slot in range(2 * RAD)]


def fourier_basis():
    points = 2.0 * np.pi * np.arange(HB_INST) / HB_INST
    basis = np.zeros((INST, INST))
    basis[0, :HB_INST] = 1.0 / np.sqrt(HB_INST)
    for wave in range(1, INST // 2):
        basis[2 * wave, :HB_INST] = np.sqrt(2.0 / HB_INST) * np.cos(wave * points)
        basis[2 * wave + 1, :HB_INST] = np.sqrt(2.0 / HB_INST) * np.sin(wave * points)
    return basis.astype(np.float32)


def halves(value):
    high = value.astype(jnp.bfloat16)
    low = (value - high.astype(jnp.float32)).astype(jnp.bfloat16)
    return high, low


def stacked(value):
    return jnp.concatenate(halves(value), axis=0)


def dot(lhs, rhs):
    return jnp.dot(lhs, rhs, preferred_element_type=jnp.float32)


def dot_nt(lhs, rhs):
    return lax.dot_general(lhs, rhs, (((1,), (1,)), ((), ())), preferred_element_type=jnp.float32)


def block_order(routes_ref, order_ref, partition, n_cell):
    blocks = routes_ref.shape[1]
    handed = blocks // 16
    above = jnp.where(partition + 1 == n_cell, 0, partition + 1)

    def place(block, heads):
        first, own, last = heads
        route = routes_ref[0, block]
        is_own = route == partition
        is_above = route == above
        position = jnp.where(is_own, own, jnp.where(is_above, first, last))
        position = jnp.minimum(position, blocks - 1)
        order_ref[0, position] = block
        one = jnp.int32(1)
        zero = jnp.int32(0)
        return (
            first + jnp.where(is_above, one, zero),
            own + jnp.where(is_own, one, zero),
            last + jnp.where(is_own | is_above, zero, one),
        )

    lax.fori_loop(0, blocks, place, (jnp.int32(0), jnp.int32(handed), jnp.int32(blocks - handed)))


def restrict_kernel(n_cell, index_ref, routes_ref, lists_ref, fine_ref, map_ref, own_ref, send_ref, order_ref, flat_ref):
    partition = index_ref[0]
    var_count, inst_dev, _ = fine_ref.shape
    blocks = map_ref.shape[0]
    rows = var_count * inst_dev
    for var in range(var_count):
        flat_ref[var * inst_dev : (var + 1) * inst_dev, :] = fine_ref[var]
    flat_ref[rows:, :] = jnp.zeros((flat_ref.shape[0] - rows, flat_ref.shape[1]), jnp.float32)
    block_order(routes_ref, order_ref, partition, n_cell)
    height = flat_ref.shape[0]
    coarse_ids = lax.broadcasted_iota(jnp.int32, (LANES, BLK), 0)
    for tile in range(blocks // PER_TILE):
        total = jnp.zeros((2 * height, LANES), jnp.float32)
        for pair in range(PER_TILE // 2):
            values = []
            hots = []
            for place in (2 * pair, 2 * pair + 1):
                block = order_ref[0, tile * PER_TILE + place]
                values.append(flat_ref[:, pl.ds(pl.multiple_of(block * BLK, BLK), BLK)])
                target = map_ref[pl.ds(block, 1), :] + place * CBLK
                hots.append(jnp.where(coarse_ids == target, 1.0, 0.0).astype(jnp.bfloat16))
            total = total + dot_nt(stacked(jnp.concatenate(values, axis=1)), jnp.concatenate(hots, axis=1))
        own_ref[:, tile * LANES : (tile + 1) * LANES] = total[:height] + total[height:]
    lane = lax.broadcasted_iota(jnp.int32, (height, LANES), 1)
    edge = blocks // 16 * CBLK
    both = jnp.where(lane < edge, own_ref[:, :LANES], own_ref[:, own_ref.shape[1] - LANES :])
    width = send_ref.shape[2]
    lists = lists_ref[...].astype(jnp.float32)
    lists = jnp.concatenate([lists, jnp.zeros((1, width - lists.shape[1]), jnp.float32)], axis=1)
    row = lax.broadcasted_iota(jnp.int32, (height, width), 0)
    wide = jnp.concatenate([both, jnp.zeros((height, width - LANES), jnp.float32)], axis=1)
    message = jnp.where(row == rows, lists, wide)
    for target in range(n_cell):
        send_ref[target] = message


def arrive_kernel(n_cell, rows, share, index_ref, got_ref, own_ref, out_ref, pack_ref):
    partition = index_ref[0]
    below = jnp.where(partition == 0, n_cell - 1, partition - 1)
    above = jnp.where(partition + 1 == n_cell, 0, partition + 1)
    height, coarse_dev = own_ref.shape
    edge = coarse_dev // 16
    lane = lax.broadcasted_iota(jnp.int32, (height, LANES), 1)
    row = lax.broadcasted_iota(jnp.int32, (height, LANES), 0)
    first = got_ref[below][:, :LANES]
    last = got_ref[above][:, :LANES]
    out_ref[...] = own_ref[...]
    out_ref[:, :LANES] = jnp.where(row < rows, jnp.where(lane < edge, first, own_ref[:, :LANES]), 0.0)
    tail = own_ref[:, coarse_dev - LANES :]
    out_ref[:, coarse_dev - LANES :] = jnp.where(row < rows, jnp.where(lane >= LANES - edge, last, tail), 0.0)
    width = pack_ref.shape[1]
    lane = lax.broadcasted_iota(jnp.int32, (1, width), 1)
    listed = jnp.full((1, width), -1.0, jnp.float32)
    for slot, offset in enumerate(OFFSETS):
        receiver = lax.rem(partition - offset + n_cell, n_cell)
        from_receiver = got_ref[receiver][rows : rows + 1, :]
        inside = (lane >= slot * share) & (lane < (slot + 1) * share)
        listed = jnp.where(inside, from_receiver, listed)
    listed = listed.astype(jnp.int32)
    ids = lax.broadcasted_iota(jnp.int32, (coarse_dev, width), 0)
    pack_ref[...] = jnp.where(ids == listed, 1.0, 0.0).astype(jnp.bfloat16)


def matrix_kernel(neighbours_ref, weights_ref, high_ref, low_ref):
    slots, coarse_dev = neighbours_ref.shape
    step = 64
    for tile in range(coarse_dev // LANES):
        span = slice(tile * LANES, (tile + 1) * LANES)
        ids = neighbours_ref[:, span]
        weights = weights_ref[:, span]

        def chunk(block, carry):
            base = pl.multiple_of(block * step, step)
            rows = lax.broadcasted_iota(jnp.int32, (step, LANES), 0) + base
            total = jnp.zeros((step, LANES), jnp.float32)
            for slot in range(slots):
                total = total + jnp.where(rows == ids[slot : slot + 1], weights[slot : slot + 1], 0.0)
            high, low = halves(total)
            high_ref[pl.ds(base, step), span] = high
            low_ref[pl.ds(base, step), span] = low
            return carry

        lax.fori_loop(0, high_ref.shape[0] // step, chunk, 0)


def swap_pairs(value):
    height = value.shape[0]
    row = lax.broadcasted_iota(jnp.int32, value.shape, 0)
    return jnp.where(row % 2 == 0, pltpu.roll(value, height - 1, 0), pltpu.roll(value, 1, 0))


def by_parity(shape, even, odd):
    row = lax.broadcasted_iota(jnp.int32, shape, 0)
    return jnp.where(row % 2 == 0, even, odd)


def pack_halo(value, pack_ref):
    packed = dot(stacked(value), pack_ref[...])
    return packed[: value.shape[0]] + packed[value.shape[0] :]


def prepare_kernel(neighbours_ref, weights_ref, spectral_ref, extra_ref,
                   high_ref, low_ref, inverse_ref, coupled_ref, topology_ref):
    matrix_kernel(neighbours_ref, weights_ref, high_ref, low_ref)
    slots, coarse_dev = neighbours_ref.shape
    var_count = extra_ref.shape[0]
    weights = weights_ref[...]
    spectral = spectral_ref[...]
    diagonal = jnp.sum(weights, axis=0, keepdims=True) + 3.0 * spectral + extra_ref[...]
    inverse = 1.0 / diagonal
    inverse_ref[...] = jnp.ones(inverse_ref.shape, jnp.float32)
    for var in range(var_count):
        inverse_ref[2 * var : 2 * var + 2, :] = jnp.broadcast_to(inverse[var : var + 1], (2, coarse_dev))
    coupled_ref[...] = by_parity(coupled_ref.shape, spectral, -spectral) * inverse_ref[...]
    topology_ref[...] = jnp.zeros(topology_ref.shape, jnp.float32)
    topology_ref[0:slots, :] = neighbours_ref[...].astype(jnp.float32)
    topology_ref[8 : 8 + slots, :] = weights
    topology_ref[16 : 16 + var_count, :] = inverse


def times(value, high, low):
    height = value.shape[0]
    extended = stacked(value)
    both = dot(extended, high)
    return both[:height] + both[height:] + dot(extended[:height], low)


def local_part(value, start_ref, inverse_ref, coupled_ref, wave, high_ref, low_ref):
    coarse_dev = value.shape[1]
    total = times(value, high_ref[:coarse_dev], low_ref[:coarse_dev])
    return start_ref[...] + total * inverse_ref[...] - wave * coupled_ref[...] * swap_pairs(value)


def begin_kernel(share, index_ref, basis_ref, gathered_ref, inverse_ref, coupled_ref, topology_ref, pack_ref, high_ref, low_ref,
                 start_ref, local_ref, send_ref):
    pair = index_ref[1]
    groups, height, coarse_dev = gathered_ref.shape
    value = jnp.zeros((height, coarse_dev), jnp.float32)
    shape = (height, coarse_dev)
    for group in range(groups):
        part = gathered_ref[group]
        straight = by_parity(shape, basis_ref[2 * pair, 2 * group], basis_ref[2 * pair + 1, 2 * group + 1])
        crossed = by_parity(shape, basis_ref[2 * pair, 2 * group + 1], basis_ref[2 * pair + 1, 2 * group])
        value = value + straight * part + crossed * swap_pairs(part)
    start = value * inverse_ref[...]
    start_ref[...] = start
    local = local_part(start, start_ref, inverse_ref, coupled_ref, pair.astype(jnp.float32), high_ref, low_ref)
    local_ref[...] = local
    send = pack_halo(jnp.concatenate([start, local, topology_ref[...]], axis=0), pack_ref)
    taller = jnp.zeros((send_ref.shape[1] - height, send.shape[1]), jnp.float32)
    everyone = jnp.concatenate([send[:height], taller], axis=0)
    next_local = jnp.concatenate([send[height : 2 * height], taller], axis=0)
    fill_send(send_ref, index_ref[0], share, everyone, (next_local, send[2 * height :]))


def fill_send(send_ref, partition, share, everyone, for_one):
    n_cell, height, width = send_ref.shape
    halo = len(OFFSETS) * share
    lane = lax.broadcasted_iota(jnp.int32, (height, width), 1)
    for target in range(n_cell):
        send_ref[target] = everyone
    for slot, offset in enumerate(OFFSETS):
        message = everyone
        for place, part in enumerate(for_one):
            begin = halo + place * share
            inside = (lane >= begin) & (lane < begin + share)
            message = jnp.where(inside, pltpu.roll(part, begin - slot * share, 1), message)
        send_ref[lax.rem(partition - offset + n_cell, n_cell)] = message


def told_of(partition, share, got_ref, place, height):
    n_cell, _, width = got_ref.shape
    lane = lax.broadcasted_iota(jnp.int32, (height, width), 1)
    begin = (len(OFFSETS) + place) * share
    told = jnp.zeros((height, width), jnp.float32)
    for slot, offset in enumerate(OFFSETS):
        sender = lax.rem(partition + offset + n_cell, n_cell)
        inside = (lane >= slot * share) & (lane < (slot + 1) * share)
        part = pltpu.roll(got_ref[sender, 0:height, :], width + slot * share - begin, 1)
        told = jnp.where(inside, part, told)
    return told


def halo_of(partition, share, got_ref, top, height):
    n_cell, _, width = got_ref.shape
    lane = lax.broadcasted_iota(jnp.int32, (height, width), 1)
    halo = jnp.zeros((height, width), jnp.float32)
    for slot, offset in enumerate(OFFSETS):
        sender = lax.rem(partition + offset + n_cell, n_cell)
        inside = (lane >= slot * share) & (lane < (slot + 1) * share)
        halo = jnp.where(inside, got_ref[sender, top : top + height, :], halo)
    return halo


def double_kernel(share, first, last, slots, var_count, *refs):
    refs = list(refs)
    index_ref, got_ref, local_ref, start_ref, inverse_ref, coupled_ref, high_ref, low_ref, pack_ref = refs[:9]
    refs = refs[9:]
    if first:
        edge_ref = None
        halo_inverse_ref = None
    else:
        edge_ref, halo_inverse_ref = refs[:2]
        refs = refs[2:]
    partition = index_ref[0]
    wave = index_ref[1].astype(jnp.float32)
    n_cell, _, width = got_ref.shape
    height, coarse_dev = local_ref.shape
    out_refs = refs
    if first:
        out_refs, (edge_ref, halo_inverse_ref) = refs[:-2], refs[-2:]
        told = told_of(partition, share, got_ref, 1, 24)
        ids = told[:slots].astype(jnp.int32) - coarse_dev
        weights = told[8 : 8 + slots]
        rows = lax.broadcasted_iota(jnp.int32, (width, width), 0)
        edge = jnp.zeros((width, width), jnp.float32)
        for slot in range(slots):
            edge = edge + jnp.where(rows == ids[slot : slot + 1], weights[slot : slot + 1], 0.0)
        high, low = halves(edge)
        edge_ref[0] = high
        edge_ref[1] = low
        halo_inverse_ref[...] = jnp.zeros((height, width), jnp.float32)
        for var in range(var_count):
            halo_inverse_ref[2 * var : 2 * var + 2, :] = jnp.broadcast_to(told[16 + var : 17 + var], (2, width))
    halo_high = high_ref[coarse_dev:]
    halo_low = low_ref[coarse_dev:]
    lane = lax.broadcasted_iota(jnp.int32, (height, width), 1)
    share_of = []
    for offset in OFFSETS:
        share_of.append(halo_of(lax.rem(partition + offset + n_cell, n_cell), share, got_ref, 0, height))
    spread = times(jnp.concatenate(share_of, axis=0), edge_ref[0], edge_ref[1])
    edge_total = jnp.zeros((height, width), jnp.float32)
    for slot in range(len(OFFSETS)):
        inside = (lane >= slot * share) & (lane < (slot + 1) * share)
        edge_total = jnp.where(inside, spread[slot * height : (slot + 1) * height], edge_total)
    next_halo = told_of(partition, share, got_ref, 0, height) + halo_inverse_ref[...] * edge_total
    both = times(
        jnp.concatenate([halo_of(partition, share, got_ref, 0, height), next_halo], axis=0), halo_high, halo_low
    )
    value = local_ref[...] + both[:height] * inverse_ref[...]
    local = local_part(value, start_ref, inverse_ref, coupled_ref, wave, high_ref, low_ref)
    value = local + both[height:] * inverse_ref[...]
    if last:
        out_ref, first_ref, last_ref = out_refs
        out_ref[...] = value
        first_ref[...] = value[:, :LANES]
        last_ref[...] = value[:, coarse_dev - LANES :]
        return
    out_ref, send_ref = out_refs
    local = local_part(value, start_ref, inverse_ref, coupled_ref, wave, high_ref, low_ref)
    out_ref[...] = local
    send = pack_halo(jnp.concatenate([value, local], axis=0), pack_ref)
    fill_send(send_ref, partition, share, send[:height], (send[height:],))


def finish_kernel(index_ref, basis_ref, order_ref, gathered_ref, map_ref, coarse_ref, fine_ref, flat_ref):
    pair = index_ref[1]
    var_count, inst_dev, coarse_dev = coarse_ref.shape
    groups, height, wide = gathered_ref.shape
    blocks = map_ref.shape[0]
    edge = blocks // 16 * CBLK
    value = jnp.zeros((height, wide), jnp.float32)
    shape = (height, wide)
    for group in range(groups):
        part = gathered_ref[group]
        straight = by_parity(shape, basis_ref[2 * group, 2 * pair], basis_ref[2 * group + 1, 2 * pair + 1])
        crossed = by_parity(shape, basis_ref[2 * group + 1, 2 * pair], basis_ref[2 * group, 2 * pair + 1])
        value = value + straight * part + crossed * swap_pairs(part)
    for var in range(var_count):
        coarse_ref[var] = value[inst_dev * var : inst_dev * (var + 1), :coarse_dev]
    lane = lax.broadcasted_iota(jnp.int32, (height, LANES), 1)
    first_back = value[:, coarse_dev + LANES : coarse_dev + 2 * LANES]
    last_back = value[:, coarse_dev : coarse_dev + LANES]
    coarse_ids = lax.broadcasted_iota(jnp.int32, (LANES, BLK), 0)
    tiles = blocks // PER_TILE
    for tile in range(tiles):
        part = value[:, tile * LANES : (tile + 1) * LANES]
        if tile == 0:
            part = jnp.where(lane < edge, last_back, part)
        if tile == tiles - 1:
            part = jnp.where(lane >= LANES - edge, first_back, part)
        part = stacked(part)
        for pair_id in range(PER_TILE // 2):
            hots = []
            spots = []
            for place in (2 * pair_id, 2 * pair_id + 1):
                block = order_ref[0, tile * PER_TILE + place]
                target = map_ref[pl.ds(block, 1), :] + place * CBLK
                hots.append(jnp.where(coarse_ids == target, 1.0, 0.0).astype(jnp.bfloat16))
                spots.append(block)
            both = dot(part, jnp.concatenate(hots, axis=1))
            both = both[:height] + both[height:]
            for place, block in enumerate(spots):
                span = pl.ds(pl.multiple_of(block * BLK, BLK), BLK)
                flat_ref[:, span] = both[:, place * BLK : (place + 1) * BLK]
    for var in range(var_count):
        fine_ref[var] = flat_ref[inst_dev * var : inst_dev * (var + 1), :]


SMEM = pl.BlockSpec(memory_space=pltpu.SMEM)
VMEM = pl.BlockSpec(memory_space=pltpu.VMEM)


def call(kernel, outs, name, in_smem, n_in, out_smem=(), scratch=(), limit=16):
    return pl.pallas_call(
        kernel,
        name=name,
        out_shape=outs,
        in_specs=[SMEM if at in in_smem else VMEM for at in range(n_in)],
        out_specs=[SMEM if at in out_smem else VMEM for at in range(len(outs))],
        scratch_shapes=list(scratch),
        compiler_params=pltpu.CompilerParams(vmem_limit_bytes=limit * MIB),
    )


def shifted(value, axis, steps):
    count = lax.axis_size(axis)
    pairs = [(source, (source + steps) % count) for source in range(count)]
    return lax.ppermute(value, axis, pairs)


def f32(*shape):
    return jax.ShapeDtypeStruct(shape, jnp.float32)


def body(fine_residual, fine_map, routes, receive_lists, neighbours, face_weights, spectral_coef, diag_extra):
    n_cell = lax.axis_size("cell")
    inst_dev, var_count, fine_dev = fine_residual.shape
    blocks = routes.shape[1]
    coarse_dev = blocks * CBLK
    rows = inst_dev * var_count
    height = -(-(rows + 1) // 16) * 16
    halo = receive_lists.shape[1]
    share = halo // (2 * RAD)
    halo_pad = -(-(halo + 2 * share) // 256) * 256
    index = jnp.stack([lax.axis_index("cell"), lax.axis_index("inst")]).astype(jnp.int32)
    basis = jnp.asarray(fourier_basis())
    cell_map = fine_map.reshape(blocks, BLK)
    fine = fine_residual.transpose(1, 0, 2)
    spectral = spectral_coef.reshape(1, coarse_dev)

    own, send, order = call(
        lambda *refs: restrict_kernel(n_cell, *refs),
        [f32(height, coarse_dev), f32(n_cell, height, halo_pad), jax.ShapeDtypeStruct((1, blocks), jnp.int32)],
        "restrict", (0, 1), 5, (2,), [pltpu.VMEM((height, fine_dev), jnp.float32)],
    )(index, routes, receive_lists, fine, cell_map)
    got = lax.all_to_all(send, "cell", 0, 0)
    arrived, pack = call(
        lambda *refs: arrive_kernel(n_cell, rows, share, *refs),
        [f32(height, coarse_dev), jax.ShapeDtypeStruct((coarse_dev, halo_pad), jnp.bfloat16)],
        "arrive", (0,), 3,
    )(index, got, own)
    gathered = lax.all_gather(arrived, "inst", axis=0)
    slots = neighbours.shape[0]
    half = jax.ShapeDtypeStruct((coarse_dev + halo_pad, coarse_dev), jnp.bfloat16)
    state = f32(height, coarse_dev)
    high, low, inverse, coupled, topology = call(
        prepare_kernel, [half, half, state, state, f32(24, coarse_dev)], "prepare", (), 4
    )(neighbours, face_weights, spectral, diag_extra)
    start, local, send = call(
        lambda *refs: begin_kernel(share, *refs), [state, state, f32(n_cell, 24, halo_pad)], "begin", (0, 1), 9
    )(index, basis, gathered, inverse, coupled, topology, pack, high, low)
    edges = []
    for pair in range(ITERS // 2):
        got = lax.all_to_all(send, "cell", 0, 0)
        is_first = pair == 0
        is_last = pair == ITERS // 2 - 1
        outs = [state, f32(n_cell, height, halo_pad)]
        if is_last:
            outs = [state, f32(height, LANES), f32(height, LANES)]
        if is_first:
            outs += [jax.ShapeDtypeStruct((2, halo_pad, halo_pad), jnp.bfloat16), f32(height, halo_pad)]
        outs = call(
            lambda *refs: double_kernel(share, is_first, is_last, slots, var_count, *refs),
            outs, "double", (0,), 9 + len(edges),
        )(index, got, local, start, inverse, coupled, high, low, pack, *edges)
        if is_first:
            edges = outs[-2:]
            outs = outs[:-2]
        local, *rest = outs
        if is_last:
            first, last = rest
        else:
            (send,) = rest
    value = local
    last_back = shifted(first, "cell", -1)
    first_back = shifted(last, "cell", 1)
    joined = jnp.concatenate([value, last_back, first_back], axis=1)
    gathered = lax.all_gather(joined, "inst", axis=0)
    coarse, fine_out = call(
        finish_kernel, [f32(var_count, inst_dev, coarse_dev), f32(var_count, inst_dev, fine_dev)],
        "finish", (0, 1, 2), 5, (), [pltpu.VMEM((height, fine_dev), jnp.float32)],
    )(index, basis, order, gathered, cell_map)
    return fine_out.transpose(1, 0, 2), coarse.transpose(1, 0, 2)


def solution(mesh):
    in_specs = (
        P("inst", None, "cell"),
        P("cell"),
        P("cell", None),
        P("cell", None),
        P(None, "cell"),
        P(None, "cell"),
        P("cell"),
        P(None, "cell"),
    )
    out_specs = (P("inst", None, "cell"), P("inst", None, "cell"))
    return jax.shard_map(body, mesh=mesh, in_specs=in_specs, out_specs=out_specs, check_vma=False)
```
